32 devices in a mesh: rep: 1 (over z), dp: 32 (over x, y, core).
Axes of the slice: x: 4, y: 4, z: 1, core: 2. Of those that a mesh axis runs over, the one named last changes fastest.
The devices are a block of a 4x4x8 slice.
Arguments:
- a: bfloat16 [32, 2, 4096, 896], P(('rep', 'dp'))
- g: bfloat16 [32, 2, 4096, 2560], P(('rep', 'dp'))
Outputs:
- output: bfloat16 [2, 896, 2560], P('rep')
All inputs are finite; a program needn't handle non-finite values.
Results may differ from the reference program's by a relative error of at most 0.012.
Values are sent between devices in bfloat16 or wider.
A program may use at most 768 MiB of HBM per device.

```python
import jax
import jax.numpy as jnp
from jax import lax

DEVICES = 32
MATRICES = 2
TOKENS = 4096
D = 896
FF = 2560


def setup_inputs(seed: int = 0, part: int = 0) -> dict:
    ka, kg, ks = (jax.random.fold_in(k, part) for k in jax.random.split(jax.random.key(seed), 3))
    size = 2.0 ** jax.random.uniform(ks, (DEVICES, MATRICES, 1, 1), jnp.float32, -1.0, 1.0)
    a = jax.random.normal(ka, (DEVICES, MATRICES, TOKENS, D), jnp.float32)
    g = size * jax.random.normal(kg, (DEVICES, MATRICES, TOKENS, FF), jnp.float32) * (DEVICES * TOKENS) ** -0.5
    return {"a": a.astype(jnp.bfloat16), "g": g.astype(jnp.bfloat16)}


def reference(a, g):
    def take(so_far, one):
        return so_far + jnp.einsum("ntd,ntf->ndf", *one, preferred_element_type=jnp.float32), None

    return lax.scan(take, jnp.zeros((MATRICES, D, FF), jnp.float32), (a, g))[0].astype(jnp.bfloat16)
```

```python
import math

import jax
import jax.numpy as jnp
from jax import lax
from jax.experimental import pallas as pl
from jax.experimental.pallas import tpu as pltpu
from jax.sharding import PartitionSpec as P

BF, F32 = jnp.bfloat16, jnp.float32
LANES = 128
A_SLOTS, G_SLOTS, P_SLOTS, RING = 4, 3, 12, 4
LAG = (0, 1, 2, 4, 5, 6, 7, 9, 10)


def kernel(side, chunk, a_ref, g_ref, out_ref, araw, at, gbuf, own, d2d_s, d2d_r, r1a_s, r1a_r, r1b_s, r1b_r, r2_s, r2_r,
           asem, gsem, send_sem, recv_sem):
    matrices, tokens, d = a_ref.shape[1:]
    per = g_ref.shape[3] // (2 * LANES)
    blocks = matrices * per
    chunks = tokens // chunk
    leaf = d // side**2

    me = lax.axis_index("dp")
    core = lax.rem(me, 2)
    y = lax.rem(me // 2, side)
    x = me // (2 * side)

    def dev(k, par):
        dx = (lax.rem(x + k + side, side) * side + y) * 2 + core
        dy = (x * side + lax.rem(y + k + side, side)) * 2 + core
        return jnp.where(par == 0, dx, dy)

    partner = me + 1 - 2 * core

    def a_copy(n, i, s):
        return pltpu.make_async_copy(a_ref.at[0, n, pl.ds(i * chunk, chunk), :], araw.at[s], asem.at[s])

    def a_turn(n, i):
        s = lax.rem(i, A_SLOTS)
        a_copy(n, i, s).wait()
        at[lax.rem(n, 2), :, pl.ds(pl.multiple_of(i * chunk, chunk), chunk)] = araw[s].T

    def g_start(b):
        s, n, j = lax.rem(b, G_SLOTS), b // per, lax.rem(b, per)
        for h, cc in ((0, core), (1, 1 - core)):
            col = pl.multiple_of((2 * j + cc) * LANES, LANES)
            pltpu.make_async_copy(
                g_ref.at[0, n, :, pl.ds(col, LANES)], gbuf.at[s, :, pl.ds(h * LANES, LANES)], gsem.at[s]
            ).start()

    def g_wait(b):
        s = lax.rem(b, G_SLOTS)
        pltpu.make_async_copy(gbuf.at[s], gbuf.at[s], gsem.at[s]).wait()

    def send(src, dst, st, b, to):
        pltpu.make_async_remote_copy(
            src_ref=src, dst_ref=dst, send_sem=send_sem.at[st, lax.rem(b, RING)], recv_sem=recv_sem.at[st, b],
            device_id={"dp": to}, device_id_type=pl.DeviceIdType.MESH,
        ).start()

    extent = (d2d_s.at[0], r1a_s.at[0], r1b_s.at[0], r2_s.at[0], r2_s.at[0], (2, side), (2, side // 2), d2d_s.at[0])

    def total(st):
        e = extent[st]
        return d2d_s.at[0, pl.ds(0, e[0] * e[1])] if isinstance(e, tuple) else e

    def wait_sent(st, b):
        pltpu.make_async_copy(total(st), total(st), send_sem.at[st, lax.rem(b, RING)]).wait()

    def wait_got(st, b):
        pltpu.make_async_copy(total(st), total(st), recv_sem.at[st, b]).wait()

    def reuse(st, b):
        @pl.when(b >= RING)
        def _():
            wait_sent(st, b)

    def at_out(b, first, count, cc):
        n, j = b // per, lax.rem(b, per)
        col = pl.multiple_of((2 * j + cc) * LANES, LANES)
        return out_ref.at[n, pl.ds(first, count), :, pl.ds(col, LANES)]

    def place(b):
        par = lax.rem(b, 2)
        return par, jnp.where(par == 0, x, y), jnp.where(par == 0, y, x), lax.rem(b, P_SLOTS), lax.rem(b, RING)

    def s0(b):
        par, pa, pb, s, r = place(b)
        g_wait(b)
        part = jnp.dot(at[lax.rem(b // per, 2)], gbuf[lax.rem(b, G_SLOTS)], preferred_element_type=F32)
        reuse(0, b)
        own[s] = part[:, :LANES].reshape(side, side, leaf, LANES)
        d2d_s[r] = part[:, LANES:].astype(BF).reshape(side**2, leaf, LANES)
        send(d2d_s.at[r], d2d_r.at[b], 0, b, partner)

    def s1(b):
        par, pa, pb, s, r = place(b)
        wait_got(0, b)
        own[s] = own[s] + d2d_r[b].reshape(side, side, leaf, LANES).astype(F32)
        reuse(1, b)
        far = lax.rem(pa + 2, side)
        r1a_s[r] = own[s, far].reshape(2, side // 2, leaf, LANES).astype(BF)
        for i, k in enumerate((1, -1)):
            send(r1a_s.at[r, i], r1a_r.at[b, i], 1, b, dev(k, par))

    def s2(b):
        par, pa, pb, s, r = place(b)
        wait_got(1, b)
        reuse(2, b)
        h = side // 2
        for i, k in enumerate((1, -1)):
            p = lax.rem(pa + k + side, side)
            r1b_s[r, i, pl.ds(i * h, h)] = (own[s, p, pl.ds(i * h, h)] + r1a_r[b, i].astype(F32)).astype(BF)
            r1b_s[r, i, pl.ds((1 - i) * h, h)] = own[s, p, pl.ds((1 - i) * h, h)].astype(BF)
            send(r1b_s.at[r, i], r1b_r.at[b, i], 2, b, dev(k, par))

    def s3(b):
        par, pa, pb, s, r = place(b)
        wait_got(2, b)
        reuse(3, b)
        own[s, pa] = own[s, pa] + r1b_r[b, 0].astype(F32) + r1b_r[b, 1].astype(F32)
        for k in range(1, side):
            r2_s[r, k - 1] = own[s, pa, lax.rem(pb + k, side)].astype(BF)
            send(r2_s.at[r, k - 1], r2_r.at[b, k - 1], 3, b, dev(k, 1 - par))

    def s4(b):
        par, pa, pb, s, r = place(b)
        wait_got(3, b)
        reuse(4, b)
        acc = own[s, pa, pb]
        for k in range(1, side):
            acc = acc + r2_r[b, k - 1].astype(F32)
        mine = at_out(b, pa * side + pb, 1, core)
        mine[...] = acc.astype(BF)[None]
        for k in range(1, side):
            send(mine, mine, 4, b, dev(k, 1 - par))

    def s5(b):
        par, pa, pb, s, r = place(b)
        wait_got(4, b)
        reuse(5, b)
        mine = at_out(b, pa * side, side, core)
        for k in (1, -1):
            send(mine, mine, 5, b, dev(k, par))

    def s6(b):
        par, pa, pb, s, r = place(b)
        wait_got(5, b)
        reuse(6, b)
        h = side // 2
        for i, k in enumerate((1, -1)):
            theirs = at_out(b, lax.rem(pa - k + side, side) * side + i * h, h, core)
            send(theirs, theirs, 6, b, dev(k, par))

    def s7(b):
        wait_got(6, b)
        reuse(7, b)
        half = at_out(b, 0, side**2, core)
        send(half, half, 7, b, partner)

    def s8(b):
        wait_got(7, b)

    g_start(0)
    for i in range(A_SLOTS):
        a_copy(0, i, i).start()
    g_start(1)
    peers = [partner] + [dev(k, par) for par in (0, 1) for k in range(1, side)]
    barrier = pltpu.get_barrier_semaphore()
    for p in peers:
        pl.semaphore_signal(barrier, inc=1, device_id={"dp": p}, device_id_type=pl.DeviceIdType.MESH)

    def first(i, _):
        a_turn(0, i)

        @pl.when(i + A_SLOTS < chunks)
        def _():
            a_copy(0, i + A_SLOTS, lax.rem(i, A_SLOTS)).start()

        return 0

    lax.fori_loop(0, chunks, first, 0)
    pl.semaphore_wait(barrier, len(peers))

    def tick(t, _):
        n, j = t // per, lax.rem(t, per)

        @pl.when((n + 1 < matrices) & (j < chunks))
        def _():
            a_copy(n + 1, j, lax.rem(j, A_SLOTS)).start()

        @pl.when(t + 2 < blocks)
        def _():
            g_start(t + 2)

        @pl.when(t < blocks)
        def _():
            s0(t)

        @pl.when((n + 1 < matrices) & (j >= 1) & (j <= chunks))
        def _():
            a_turn(n + 1, j - 1)

        for st, lag in reversed(list(enumerate((s1, s2, s3, s4, s5, s6, s7, s8), 1))):
            b = t - LAG[st]

            @pl.when((b >= 0) & (b < blocks))
            def _():
                lag(b)

        return 0

    lax.fori_loop(0, blocks + LAG[-1], tick, 0)

    def drain(b, _):
        for st in range(8):
            wait_sent(st, b)
        return 0

    lax.fori_loop(blocks - RING, blocks, drain, 0)


def solution(mesh):
    side = math.isqrt(mesh.shape["dp"] // 2)

    def step(a, g):
        matrices, tokens, d = a.shape[1:]
        f = g.shape[3]
        leaf, blocks = d // side**2, matrices * f // (2 * LANES)
        chunk = tokens // 8
        quarter, h = (side, leaf, LANES), side // 2
        out = pl.pallas_call(
            lambda *refs: kernel(side, chunk, *refs),
            out_shape=OUT((matrices, side**2, leaf, f), BF),
            in_specs=[pl.BlockSpec(memory_space=pl.ANY)] * 2,
            out_specs=pl.BlockSpec(memory_space=OUT_SPACE),
            scratch_shapes=[
                pltpu.VMEM((A_SLOTS, chunk, d), BF),
                pltpu.VMEM((2, d, tokens), BF),
                pltpu.VMEM((G_SLOTS, tokens, 2 * LANES), BF),
                pltpu.VMEM((P_SLOTS, side, *quarter), F32),
                pltpu.VMEM((RING, side**2, leaf, LANES), BF),
                pltpu.VMEM((blocks, side**2, leaf, LANES), BF),
                pltpu.VMEM((RING, 2, h, leaf, LANES), BF),
                pltpu.VMEM((blocks, 2, h, leaf, LANES), BF),
                pltpu.VMEM((RING, 2, *quarter), BF),
                pltpu.VMEM((blocks, 2, *quarter), BF),
                pltpu.VMEM((RING, side - 1, leaf, LANES), BF),
                pltpu.VMEM((blocks, side - 1, leaf, LANES), BF),
                pltpu.SemaphoreType.DMA((A_SLOTS,)),
                pltpu.SemaphoreType.DMA((G_SLOTS,)),
                pltpu.SemaphoreType.DMA((8, RING)),
                pltpu.SemaphoreType.DMA((8, blocks)),
            ],
            compiler_params=pltpu.CompilerParams(
                collective_id=0, has_side_effects=True, vmem_limit_bytes=50 * 2**20
            ),
            name="sums",
        )(a, g)
        return out.reshape(matrices, d, f)

    spec = P(("rep", "dp"))
    return jax.shard_map(step, mesh=mesh, in_specs=(spec, spec), out_specs=P("rep"), check_vma=False)


OUT, OUT_SPACE = pltpu.VMEM, pltpu.VMEM
```

```python
import math

import jax
import jax.numpy as jnp
from jax import lax
from jax.experimental import pallas as pl
from jax.experimental.pallas import tpu as pltpu
from jax.sharding import PartitionSpec as P

BF, F32 = jnp.bfloat16, jnp.float32
LANES = 128
G_SLOTS, RING = 3, 8
LAG = (0, 1, 3, 6, 8, 10, 13, 15, 16)
FAST = 6
FLAG = (0, 1, 4, 6, 8, 11, 12)
P_SLOTS = max(LAG[4], FLAG[3]) + 1
STAGES = 10


def kernel(side, chunk, a_ref, g_ref, out_ref, araw, at0, at1, gbuf, own, d2d_s, d2d_r, r1a_s, r1a_r, r1b_s, r1b_r, r2a_s, r2a_r, r2b_s, r2b_r,
           asem, gsem, send_sem, recv_sem):
    matrices, tokens, d = a_ref.shape[1:]
    per = g_ref.shape[3] // (2 * LANES)
    blocks = matrices * per
    chunks = tokens // chunk
    leaf = d // side**2

    me = lax.axis_index("dp")
    core = lax.rem(me, 2)
    y = lax.rem(me // 2, side)
    x = me // (2 * side)

    def dev(k, par):
        dx = (lax.rem(x + k + side, side) * side + y) * 2 + core
        dy = (x * side + lax.rem(y + k + side, side)) * 2 + core
        return jnp.where(par == 0, dx, dy)

    partner = me + 1 - 2 * core

    def a_copy(n, i):
        return pltpu.make_async_copy(a_ref.at[0, n, pl.ds(i * chunk, chunk), :], araw.at[i], asem.at[i])

    at = (at0, at1)

    def a_turn(n, i):
        at[n % 2][:, pl.ds(pl.multiple_of(i * chunk, chunk), chunk)] = araw[i].T

    def split(b):
        n = sum((b >= k * per).astype(jnp.int32) for k in range(1, matrices)) + jnp.int32(0)
        return n, b - n * per

    def g_start(b):
        s = lax.rem(b, G_SLOTS)
        n, j = split(b)
        for h, cc in ((0, core), (1, 1 - core)):
            col = pl.multiple_of((2 * j + cc) * LANES, LANES)
            pltpu.make_async_copy(
                g_ref.at[0, n, :, pl.ds(col, LANES)], gbuf.at[s, :, pl.ds(h * LANES, LANES)], gsem.at[s]
            ).start()

    def g_wait(b):
        s = lax.rem(b, G_SLOTS)
        pltpu.make_async_copy(gbuf.at[s], gbuf.at[s], gsem.at[s]).wait()

    def send(src, dst, st, b, to):
        pltpu.make_async_remote_copy(
            src_ref=src, dst_ref=dst, send_sem=send_sem.at[st, lax.rem(b, RING)], recv_sem=recv_sem.at[st, b],
            device_id={"dp": to}, device_id_type=pl.DeviceIdType.MESH,
        ).start()

    extent = (
        d2d_s.at[0], r1a_s.at[0], r1b_s.at[0], r2a_s.at[0], r2b_s.at[0], r2b_s.at[0], r2a_s.at[0],
        (2, side), (2, side // 2), d2d_s.at[0],
    )

    def total(st):
        e = extent[st]
        return d2d_s.at[0, pl.ds(0, e[0] * e[1])] if isinstance(e, tuple) else e

    def wait_sent(st, b):
        pltpu.make_async_copy(total(st), total(st), send_sem.at[st, lax.rem(b, RING)]).wait()

    def wait_got(st, b):
        pltpu.make_async_copy(total(st), total(st), recv_sem.at[st, b]).wait()

    def reuse(st, b):
        @pl.when(b >= RING)
        def _():
            wait_sent(st, b)

    def at_out(b, first, count, cc):
        n, j = split(b)
        col = pl.multiple_of((2 * j + cc) * LANES, LANES)
        return out_ref.at[n, pl.ds(first, count), :, pl.ds(col, LANES)]

    def place(b):
        par = lax.rem(b, 2)
        return par, jnp.where(par == 0, x, y), jnp.where(par == 0, y, x), lax.rem(b, P_SLOTS), lax.rem(b, RING)

    peers = [partner] + [dev(k, par) for par in (0, 1) for k in range(1, side)]
    barrier = pltpu.get_barrier_semaphore()

    def s0(n, b, turn):
        par, pa, pb, s, r = place(b)
        j = split(b)[1]
        g_wait(b)
        if turn:
            a_copy(n + 1, j - 1).wait()
        reuse(0, b)
        part = jnp.dot(at[n % 2][...], gbuf[lax.rem(b, G_SLOTS)], preferred_element_type=F32)
        if turn:
            a_turn(n + 1, j - 1)
        own[s] = part[:, :LANES].reshape(side, side, leaf, LANES)
        d2d_s[r] = part[:, LANES:].astype(BF).reshape(side**2, leaf, LANES)
        if n == 0:

            @pl.when(b == 0)
            def _():
                pl.semaphore_wait(barrier, len(peers))

        send(d2d_s.at[r], d2d_r.at[b], 0, b, partner)

    def s1(b):
        par, pa, pb, s, r = place(b)
        wait_got(0, b)
        own[s] = own[s] + d2d_r[b].reshape(side, side, leaf, LANES).astype(F32)
        reuse(1, b)
        far = lax.rem(pa + 2, side)
        r1a_s[r] = own[s, far].reshape(2, side // 2, leaf, LANES).astype(BF)
        for i, k in enumerate((1, -1)):
            send(r1a_s.at[r, i], r1a_r.at[b, i], 1, b, dev(k, par))

    def s2(b):
        par, pa, pb, s, r = place(b)
        wait_got(1, b)
        reuse(2, b)
        h = side // 2
        for i, k in enumerate((1, -1)):
            p = lax.rem(pa + k + side, side)
            r1b_s[r, i, pl.ds(i * h, h)] = (own[s, p, pl.ds(i * h, h)] + r1a_r[b, i].astype(F32)).astype(BF)
            r1b_s[r, i, pl.ds((1 - i) * h, h)] = own[s, p, pl.ds((1 - i) * h, h)].astype(BF)
            send(r1b_s.at[r, i], r1b_r.at[b, i], 2, b, dev(k, par))

    def s3(b):
        par, pa, pb, s, r = place(b)
        wait_got(2, b)
        own[s, pa] = own[s, pa] + r1b_r[b, 0].astype(F32) + r1b_r[b, 1].astype(F32)
        leaves(b)

    def leaves(b):
        par, pa, pb, s, r = place(b)
        reuse(3, b)
        reuse(4, b)
        r2a_s[r, 0] = own[s, pa, lax.rem(pb + 2, side)].astype(BF)
        send(r2a_s.at[r, 0], r2a_r.at[b, 0], 3, b, dev(2, 1 - par))
        for i, k in enumerate((1, -1)):
            r2b_s[r, i] = own[s, pa, lax.rem(pb + k + side, side)].astype(BF)
            send(r2b_s.at[r, i], r2b_r.at[b, i], 4, b, dev(k, 1 - par))

    def s4(b):
        par, pa, pb, s, r = place(b)
        wait_got(3, b)
        wait_got(4, b)
        reuse(5, b)
        reuse(6, b)
        mine = at_out(b, pa * side + pb, 1, core)
        got = r2b_r[b, 0].astype(F32) + r2b_r[b, 1].astype(F32) + r2a_r[b, 0].astype(F32)
        mine[...] = (own[s, pa, pb] + got).astype(BF)[None]
        send(mine, mine, 6, b, dev(2, 1 - par))
        for k in (1, -1):
            send(mine, mine, 5, b, dev(k, 1 - par))

    def s5(b):
        par, pa, pb, s, r = place(b)
        wait_got(5, b)
        wait_got(6, b)
        reuse(7, b)
        mine = at_out(b, pa * side, side, core)
        for k in (1, -1):
            send(mine, mine, 7, b, dev(k, par))

    def s6(b):
        par, pa, pb, s, r = place(b)
        wait_got(7, b)
        reuse(8, b)
        h = side // 2
        for i, k in enumerate((1, -1)):
            theirs = at_out(b, lax.rem(pa - k + side, side) * side + i * h, h, core)
            send(theirs, theirs, 8, b, dev(k, par))

    def s7(b):
        wait_got(8, b)
        reuse(9, b)
        half = at_out(b, 0, side**2, core)
        send(half, half, 9, b, partner)

    def s8(b):
        wait_got(9, b)

    def f1(b):
        par, pa, pb, s, r = place(b)
        wait_got(0, b)
        own[s] = own[s] + d2d_r[b].reshape(side, side, leaf, LANES).astype(F32)
        reuse(1, b)
        reuse(2, b)
        r1a_s[r] = own[s, lax.rem(pa + 2, side)].reshape(2, side // 2, leaf, LANES).astype(BF)
        send(r1a_s.at[r], r1a_r.at[b], 1, b, dev(2, par))
        for i, k in enumerate((1, -1)):
            r1b_s[r, i] = own[s, lax.rem(pa + k + side, side)].astype(BF)
            send(r1b_s.at[r, i], r1b_r.at[b, i], 2, b, dev(k, par))

    def f2(b):
        par, pa, pb, s, r = place(b)
        wait_got(1, b)
        wait_got(2, b)
        got = r1a_r[b].reshape(side, leaf, LANES).astype(F32)
        own[s, pa] = own[s, pa] + r1b_r[b, 0].astype(F32) + r1b_r[b, 1].astype(F32) + got
        leaves(b)

    def f4(b):
        par, pa, pb, s, r = place(b)
        wait_got(5, b)
        wait_got(6, b)
        reuse(7, b)
        reuse(8, b)
        mine = at_out(b, pa * side, side, core)
        send(mine, mine, 8, b, dev(2, par))
        for k in (1, -1):
            send(mine, mine, 7, b, dev(k, par))

    def f5(b):
        wait_got(7, b)
        s7(b)

    g_start(jnp.int32(0))
    for i in range(chunks):
        a_copy(0, i).start()
    g_start(jnp.int32(1))
    for p in peers:
        pl.semaphore_signal(barrier, inc=1, device_id={"dp": p}, device_id_type=pl.DeviceIdType.MESH)

    def first(i, _):
        a_copy(0, i).wait()
        a_turn(0, i)
        return 0

    lax.fori_loop(0, chunks, first, 0)

    def later(t):
        for st, stage in reversed(list(enumerate((s1, s2, s3, s4, s5, s6, s7, s8), 1))):
            b = t - LAG[st]

            @pl.when((b >= 0) & (b < blocks - FAST))
            def _():
                stage(b)

        for st, stage in reversed(list(enumerate((f1, f2, s4, f4, f5, s8), 1))):
            b = t - FLAG[st]

            @pl.when((b >= blocks - FAST) & (b < blocks))
            def _():
                stage(b)

    for n in range(matrices):
        turns = n + 1 < matrices

        def tick(t, _):
            j = t - n * per
            if turns:

                @pl.when(j < chunks)
                def _():
                    a_copy(n + 1, j).start()

            @pl.when(t + 2 < blocks)
            def _():
                g_start(t + 2)

            if turns:
                busy = (j >= 1) & (j <= chunks)

                @pl.when(busy)
                def _():
                    s0(n, t, True)

                @pl.when(jnp.logical_not(busy))
                def _():
                    s0(n, t, False)
            else:
                s0(n, t, False)
            later(t)
            return 0

        lax.fori_loop(n * per, (n + 1) * per, tick, 0)

    def tail(t, _):
        later(t)
        return 0

    lax.fori_loop(blocks, blocks + max(LAG[-1] - FAST, FLAG[-1]), tail, 0)

    def drain(b, _):
        for st in range(STAGES):
            wait_sent(st, b)
        return 0

    lax.fori_loop(blocks - RING, blocks, drain, 0)


def solution(mesh):
    side = math.isqrt(mesh.shape["dp"] // 2)

    def step(a, g):
        matrices, tokens, d = a.shape[1:]
        f = g.shape[3]
        leaf, blocks = d // side**2, matrices * f // (2 * LANES)
        chunk = tokens // 8
        quarter, h = (side, leaf, LANES), side // 2
        out = pl.pallas_call(
            lambda *refs: kernel(side, chunk, *refs),
            out_shape=OUT((matrices, side**2, leaf, f), BF),
            in_specs=[pl.BlockSpec(memory_space=pl.ANY)] * 2,
            out_specs=pl.BlockSpec(memory_space=OUT_SPACE),
            scratch_shapes=[
                pltpu.VMEM((8, chunk, d), BF),
                pltpu.VMEM((d, tokens), BF),
                pltpu.VMEM((d, tokens), BF),
                pltpu.VMEM((G_SLOTS, tokens, 2 * LANES), BF),
                pltpu.VMEM((P_SLOTS, side, *quarter), F32),
                pltpu.VMEM((RING, side**2, leaf, LANES), BF),
                pltpu.VMEM((blocks, side**2, leaf, LANES), BF),
                pltpu.VMEM((RING, 2, h, leaf, LANES), BF),
                pltpu.VMEM((blocks, 2, h, leaf, LANES), BF),
                pltpu.VMEM((RING, 2, *quarter), BF),
                pltpu.VMEM((blocks, 2, *quarter), BF),
                pltpu.VMEM((RING, 1, leaf, LANES), BF),
                pltpu.VMEM((blocks, 1, leaf, LANES), BF),
                pltpu.VMEM((RING, 2, leaf, LANES), BF),
                pltpu.VMEM((blocks, 2, leaf, LANES), BF),
                pltpu.SemaphoreType.DMA((8,)),
                pltpu.SemaphoreType.DMA((G_SLOTS,)),
                pltpu.SemaphoreType.DMA((STAGES, RING)),
                pltpu.SemaphoreType.DMA((STAGES, blocks)),
            ],
            compiler_params=pltpu.CompilerParams(
                collective_id=0, has_side_effects=True, vmem_limit_bytes=53 * 2**20
            ),
            name="sums",
        )(a, g)
        return out.reshape(matrices, d, f)

    spec = P(("rep", "dp"))
    return jax.shard_map(step, mesh=mesh, in_specs=(spec, spec), out_specs=P("rep"), check_vma=False)


OUT, OUT_SPACE = pltpu.VMEM, pltpu.VMEM
```

```python
import math

import jax
import jax.numpy as jnp
from jax import lax
from jax.experimental import pallas as pl
from jax.experimental.pallas import tpu as pltpu
from jax.sharding import PartitionSpec as P

BF, F32 = jnp.bfloat16, jnp.float32
LANES = 128
G_SLOTS, RING = 3, 8
LAG = (0, 1, 3, 5, 7, 9, 12, 14, 15)
FAST = 6
FLAG = (0, 1, 4, 6, 8, 11, 12)
P_SLOTS = max(LAG[4], FLAG[3]) + 1
STAGES = 10


def kernel(side, chunk, a_ref, g_ref, out_ref, araw, at0, at1, gbuf, own, d2d_s, d2d_r, r1a_s, r1a_r, r1b_s, r1b_r, r2a_s, r2a_r, r2b_s, r2b_r,
           asem, gsem, send_sem, recv_sem):
    matrices, tokens, d = a_ref.shape[1:]
    per = g_ref.shape[3] // (2 * LANES)
    blocks = matrices * per
    chunks = tokens // chunk
    leaf = d // side**2

    me = lax.axis_index("dp")
    core = lax.rem(me, 2)
    y = lax.rem(me // 2, side)
    x = me // (2 * side)

    place_at = {k: (lax.rem(x + k + side, side), lax.rem(y + k + side, side)) for k in (0, 1, 2, -1)}
    device_at = {k: ((px * side + y) * 2 + core, (x * side + py) * 2 + core) for k, (px, py) in place_at.items()}

    def pick(xy, par):
        return jnp.where(par == 0, *xy)

    def dev(k, par):
        return pick(device_at[k], par)

    def ring(k, par):
        return pick(place_at[k], par)

    partner = me + 1 - 2 * core

    def a_copy(n, i):
        return pltpu.make_async_copy(a_ref.at[0, n, pl.ds(i * chunk, chunk), :], araw.at[i], asem.at[i])

    at = (at0, at1)

    def a_turn(n, i):
        at[n % 2][:, pl.ds(pl.multiple_of(i * chunk, chunk), chunk)] = araw[i].T

    def split(b):
        n = sum((b >= k * per).astype(jnp.int32) for k in range(1, matrices)) + jnp.int32(0)
        return n, b - n * per

    def g_start(b):
        s = lax.rem(b, G_SLOTS)
        n, j = split(b)
        for h, cc in ((0, core), (1, 1 - core)):
            col = pl.multiple_of((2 * j + cc) * LANES, LANES)
            pltpu.make_async_copy(
                g_ref.at[0, n, :, pl.ds(col, LANES)], gbuf.at[s, :, pl.ds(h * LANES, LANES)], gsem.at[s]
            ).start()

    def g_wait(b):
        s = lax.rem(b, G_SLOTS)
        pltpu.make_async_copy(gbuf.at[s], gbuf.at[s], gsem.at[s]).wait()

    def send(src, dst, st, b, to):
        pltpu.make_async_remote_copy(
            src_ref=src, dst_ref=dst, send_sem=send_sem.at[st, lax.rem(b, RING)], recv_sem=recv_sem.at[st, b],
            device_id={"dp": to}, device_id_type=pl.DeviceIdType.MESH,
        ).start()

    extent = (
        d2d_s.at[0], r1a_s.at[0], r1b_s.at[0], r2a_s.at[0], r2b_s.at[0], r2b_s.at[0], r2a_s.at[0],
        (2, side), (2, side // 2), d2d_s.at[0],
    )

    def total(st):
        e = extent[st]
        return d2d_s.at[0, pl.ds(0, e[0] * e[1])] if isinstance(e, tuple) else e

    def wait_sent(st, b):
        pltpu.make_async_copy(total(st), total(st), send_sem.at[st, lax.rem(b, RING)]).wait()

    def wait_got(st, b):
        pltpu.make_async_copy(total(st), total(st), recv_sem.at[st, b]).wait()

    def reuse(st, b):
        @pl.when(b >= RING)
        def _():
            wait_sent(st, b)

    def at_out(b, first, count, cc):
        n, j = split(b)
        col = pl.multiple_of((2 * j + cc) * LANES, LANES)
        return out_ref.at[n, pl.ds(first, count), :, pl.ds(col, LANES)]

    def place(b):
        par = lax.rem(b, 2)
        return par, jnp.where(par == 0, x, y), jnp.where(par == 0, y, x), lax.rem(b, P_SLOTS), lax.rem(b, RING)

    peers = [partner] + [dev(k, par) for par in (0, 1) for k in (1, 2, -1)]
    barrier = pltpu.get_barrier_semaphore()

    def s0(n, b, turn):
        par, pa, pb, s, r = place(b)
        j = split(b)[1]
        g_wait(b)
        if turn:
            a_copy(n + 1, j - 1).wait()
        reuse(0, b)
        part = jnp.dot(at[n % 2][...], gbuf[lax.rem(b, G_SLOTS)], preferred_element_type=F32)
        if turn:
            a_turn(n + 1, j - 1)
        own[s] = part[:, :LANES].reshape(side, side, leaf, LANES)
        d2d_s[r] = part[:, LANES:].astype(BF).reshape(side**2, leaf, LANES)
        if n == 0:

            @pl.when(b == 0)
            def _():
                pl.semaphore_wait(barrier, len(peers))

        send(d2d_s.at[r], d2d_r.at[b], 0, b, partner)

    def s1(b):
        par, pa, pb, s, r = place(b)
        wait_got(0, b)
        own[s] = own[s] + d2d_r[b].reshape(side, side, leaf, LANES).astype(F32)
        reuse(1, b)
        far = ring(2, par)
        r1a_s[r] = own[s, far].reshape(2, side // 2, leaf, LANES).astype(BF)
        for i, k in enumerate((1, -1)):
            send(r1a_s.at[r, i], r1a_r.at[b, i], 1, b, dev(k, par))

    def s2(b):
        par, pa, pb, s, r = place(b)
        wait_got(1, b)
        reuse(2, b)
        h = side // 2
        for i, k in enumerate((1, -1)):
            p = ring(k, par)
            r1b_s[r, i, pl.ds(i * h, h)] = (own[s, p, pl.ds(i * h, h)] + r1a_r[b, i].astype(F32)).astype(BF)
            r1b_s[r, i, pl.ds((1 - i) * h, h)] = own[s, p, pl.ds((1 - i) * h, h)].astype(BF)
            send(r1b_s.at[r, i], r1b_r.at[b, i], 2, b, dev(k, par))

    def s3(b):
        par, pa, pb, s, r = place(b)
        wait_got(2, b)
        own[s, pa] = own[s, pa] + r1b_r[b, 0].astype(F32) + r1b_r[b, 1].astype(F32)
        leaves(b)

    def leaves(b):
        par, pa, pb, s, r = place(b)
        reuse(3, b)
        reuse(4, b)
        r2a_s[r, 0] = own[s, pa, ring(2, 1 - par)].astype(BF)
        send(r2a_s.at[r, 0], r2a_r.at[b, 0], 3, b, dev(2, 1 - par))
        for i, k in enumerate((1, -1)):
            r2b_s[r, i] = own[s, pa, ring(k, 1 - par)].astype(BF)
            send(r2b_s.at[r, i], r2b_r.at[b, i], 4, b, dev(k, 1 - par))

    def s4(b):
        par, pa, pb, s, r = place(b)
        wait_got(3, b)
        wait_got(4, b)
        reuse(5, b)
        reuse(6, b)
        mine = at_out(b, pa * side + pb, 1, core)
        got = r2b_r[b, 0].astype(F32) + r2b_r[b, 1].astype(F32) + r2a_r[b, 0].astype(F32)
        mine[...] = (own[s, pa, pb] + got).astype(BF)[None]
        send(mine, mine, 6, b, dev(2, 1 - par))
        for k in (1, -1):
            send(mine, mine, 5, b, dev(k, 1 - par))

    def s5(b):
        par, pa, pb, s, r = place(b)
        wait_got(5, b)
        wait_got(6, b)
        reuse(7, b)
        mine = at_out(b, pa * side, side, core)
        for k in (1, -1):
            send(mine, mine, 7, b, dev(k, par))

    def s6(b):
        par, pa, pb, s, r = place(b)
        wait_got(7, b)
        reuse(8, b)
        h = side // 2
        for i, k in enumerate((1, -1)):
            theirs = at_out(b, ring(-k, par) * side + i * h, h, core)
            send(theirs, theirs, 8, b, dev(k, par))

    def s7(b):
        wait_got(8, b)
        reuse(9, b)
        half = at_out(b, 0, side**2, core)
        send(half, half, 9, b, partner)

    def s8(b):
        wait_got(9, b)

    def f1(b):
        par, pa, pb, s, r = place(b)
        wait_got(0, b)
        own[s] = own[s] + d2d_r[b].reshape(side, side, leaf, LANES).astype(F32)
        reuse(1, b)
        reuse(2, b)
        r1a_s[r] = own[s, ring(2, par)].reshape(2, side // 2, leaf, LANES).astype(BF)
        send(r1a_s.at[r], r1a_r.at[b], 1, b, dev(2, par))
        for i, k in enumerate((1, -1)):
            r1b_s[r, i] = own[s, ring(k, par)].astype(BF)
            send(r1b_s.at[r, i], r1b_r.at[b, i], 2, b, dev(k, par))

    def f2(b):
        par, pa, pb, s, r = place(b)
        wait_got(1, b)
        wait_got(2, b)
        got = r1a_r[b].reshape(side, leaf, LANES).astype(F32)
        own[s, pa] = own[s, pa] + r1b_r[b, 0].astype(F32) + r1b_r[b, 1].astype(F32) + got
        leaves(b)

    def f4(b):
        par, pa, pb, s, r = place(b)
        wait_got(5, b)
        wait_got(6, b)
        reuse(7, b)
        reuse(8, b)
        mine = at_out(b, pa * side, side, core)
        send(mine, mine, 8, b, dev(2, par))
        for k in (1, -1):
            send(mine, mine, 7, b, dev(k, par))

    def f5(b):
        wait_got(7, b)
        s7(b)

    for i in range(chunks):
        a_copy(0, i).start()
    g_start(jnp.int32(0))
    g_start(jnp.int32(1))
    for p in peers:
        pl.semaphore_signal(barrier, inc=1, device_id={"dp": p}, device_id_type=pl.DeviceIdType.MESH)

    def first(i, _):
        a_copy(0, i).wait()
        a_turn(0, i)
        return 0

    lax.fori_loop(0, chunks, first, 0)

    def later(t):
        for first_b, last_b, lags, stages in (
            (0, blocks - FAST, LAG, (s1, s2, s3, s4, s5, s6, s7, s8)),
            (blocks - FAST, blocks, FLAG, (f1, f2, s4, f4, f5, s8)),
        ):

            @pl.when((t >= first_b + lags[1]) & (t < last_b + lags[-1]))
            def _():
                for st, stage in reversed(list(enumerate(stages, 1))):
                    b = t - lags[st]

                    @pl.when((b >= first_b) & (b < last_b))
                    def _():
                        stage(b)

    for n in range(matrices):
        turns = n + 1 < matrices

        def tick(t, _):
            j = t - n * per
            if turns:

                @pl.when(j < chunks)
                def _():
                    a_copy(n + 1, j).start()

            @pl.when(t + 2 < blocks)
            def _():
                g_start(t + 2)

            if turns:
                busy = (j >= 1) & (j <= chunks)

                @pl.when(busy)
                def _():
                    s0(n, t, True)

                @pl.when(jnp.logical_not(busy))
                def _():
                    s0(n, t, False)
            else:
                s0(n, t, False)
            later(t)
            return 0

        lax.fori_loop(n * per, (n + 1) * per, tick, 0)

    def tail(t, _):
        later(t)
        return 0

    lax.fori_loop(blocks, blocks + max(LAG[-1] - FAST, FLAG[-1]), tail, 0)

    def drain(b, _):
        for st in range(STAGES):
            wait_sent(st, b)
        return 0

    lax.fori_loop(blocks - RING, blocks, drain, 0)


def solution(mesh):
    side = math.isqrt(mesh.shape["dp"] // 2)

    def step(a, g):
        matrices, tokens, d = a.shape[1:]
        f = g.shape[3]
        leaf, blocks = d // side**2, matrices * f // (2 * LANES)
        chunk = tokens // 8
        quarter, h = (side, leaf, LANES), side // 2
        out = pl.pallas_call(
            lambda *refs: kernel(side, chunk, *refs),
            out_shape=OUT((matrices, side**2, leaf, f), BF),
            in_specs=[pl.BlockSpec(memory_space=pl.ANY)] * 2,
            out_specs=pl.BlockSpec(memory_space=OUT_SPACE),
            scratch_shapes=[
                pltpu.VMEM((8, chunk, d), BF),
                pltpu.VMEM((d, tokens), BF),
                pltpu.VMEM((d, tokens), BF),
                pltpu.VMEM((G_SLOTS, tokens, 2 * LANES), BF),
                pltpu.VMEM((P_SLOTS, side, *quarter), F32),
                pltpu.VMEM((RING, side**2, leaf, LANES), BF),
                pltpu.VMEM((blocks, side**2, leaf, LANES), BF),
                pltpu.VMEM((RING, 2, h, leaf, LANES), BF),
                pltpu.VMEM((blocks, 2, h, leaf, LANES), BF),
                pltpu.VMEM((RING, 2, *quarter), BF),
                pltpu.VMEM((blocks, 2, *quarter), BF),
                pltpu.VMEM((RING, 1, leaf, LANES), BF),
                pltpu.VMEM((blocks, 1, leaf, LANES), BF),
                pltpu.VMEM((RING, 2, leaf, LANES), BF),
                pltpu.VMEM((blocks, 2, leaf, LANES), BF),
                pltpu.SemaphoreType.DMA((8,)),
                pltpu.SemaphoreType.DMA((G_SLOTS,)),
                pltpu.SemaphoreType.DMA((STAGES, RING)),
                pltpu.SemaphoreType.DMA((STAGES, blocks)),
            ],
            compiler_params=pltpu.CompilerParams(
                collective_id=0, has_side_effects=True, vmem_limit_bytes=53 * 2**20
            ),
            name="sums",
        )(a, g)
        return out.reshape(matrices, d, f)

    spec = P(("rep", "dp"))
    return jax.shard_map(step, mesh=mesh, in_specs=(spec, spec), out_specs=P("rep"), check_vma=False)


OUT, OUT_SPACE = pltpu.VMEM, pltpu.VMEM
```
